32 devices in a mesh: panel: 4 (over x, core), tile: 8 (over z, y).
Axes of the slice: x: 2, y: 2, z: 4, core: 2. Of those that a mesh axis runs over, the one named last changes fastest.
Arguments:
- residual: float32 [4, 8, 16, 8, 128], P('panel', 'tile'), may hold values from -6 to 6
- inverse: bfloat16 [4, 8, 2, 576, 576], P('panel', 'tile'), may hold values from -1 to 2
- blend_weight: float32 [576], replicated, may hold values from 0.1 to 1.9
- seam_table: int32 [4, 4, 3], replicated, may hold values from -1 to 3, as said below
Outputs:
- correction: float32 [4, 8, 16, 8, 128], P('panel', 'tile')
The draws below stay inside these ranges and needn't reach their ends.
Inputs may be any that keep to these rules, and one draw needn't show every extreme that they name: seam_table[p, e] holds the neighbour panel across edge e of panel p (or -1), a rotation r and a reversal v. Every panel has neighbours across exactly two opposite edges (0 and 2, or 1 and 3) and the entries -1, 0, 0 on the other two; the panels form one closed cycle and each panel's two neighbours differ. If edge e of p faces panel q, then edge c = (e + 2 + r) mod 4 of q faces p with rotation (-r) mod 4 and the same reversal v. At least one seam joins edge 0 of a panel to edge 0 of another, with rotation 2 and reversal 1.
All inputs are finite; a program needn't handle non-finite values.
Results may differ from the reference program's by a relative error of at most 0.0029.
Values may be sent and summed in bfloat16 or wider, within the bound.
A program may use at most 128 MiB of HBM per device.

```python
import math
import jax
import jax.numpy as jnp
from jax import lax

PANELS = 4
SUB = 8
INTERSECTION = 8
COLS = 128
TILES = 8
TILE_COLS = 4
TILE_W = 8
TILE_H = 16
NSUB = 2
CELLS = 576


def draw_inverse(key, part):
    matrix_order = CELLS

    def one_block(tile_index):
        sub_key = jax.random.fold_in(key, tile_index)
        noise_part = jax.random.normal(jax.random.fold_in(sub_key, 3), (NSUB, matrix_order, matrix_order), jnp.float32)
        noise_part = noise_part * (0.6 / math.sqrt(matrix_order))
        diagonal = jax.random.uniform(jax.random.fold_in(sub_key, 4), (NSUB, matrix_order), jnp.float32, 0.5, 1.5)
        result = noise_part + diagonal[:, :, None] * jnp.eye(matrix_order, dtype=jnp.float32)[None]
        return result.astype(jnp.bfloat16)
    blocks = lax.map(one_block, jnp.arange(PANELS * TILES, dtype=jnp.int32))
    return blocks.reshape(PANELS, TILES, NSUB, matrix_order, matrix_order)


def draw_seam_table(key, part):
    ordering = jax.random.permutation(jax.random.fold_in(key, 1), PANELS).astype(jnp.int32)
    rotations = jax.random.randint(jax.random.fold_in(key, 2), (PANELS,), 0, 4).astype(jnp.int32)
    rotations = rotations.at[ordering[0]].set(2)
    rotations = rotations.at[ordering[1]].set(0)
    direction = jnp.array([1, -1, -1, 1], jnp.int32)
    seam_grid = jnp.zeros((PANELS, 4, 3), jnp.int32).at[:, :, 0].set(-1)
    for position in range(PANELS):
        current = ordering[position]
        following = ordering[(position + 1) % PANELS]
        east_edge = (2 + rotations[current]) % 4
        west_edge = rotations[following] % 4
        reversal = (direction[rotations[current]] != direction[rotations[following]]).astype(jnp.int32)
        seam_grid = seam_grid.at[current, east_edge].set(jnp.stack([following, (west_edge - east_edge - 2) % 4, reversal]))
        seam_grid = seam_grid.at[following, west_edge].set(jnp.stack([current, (east_edge - west_edge - 2) % 4, reversal]))
    return seam_grid


def steps_of(own_key, dims, shards, least, top_value):
    level = 1.0
    for dim, blocks in shards:
        steps = jax.random.uniform(jax.random.fold_in(jax.random.fold_in(own_key, 6), dim), (blocks,), jnp.float32, least / len(shards), top_value / len(shards))
        level = level * jnp.repeat(jnp.exp(steps), dims[dim] // blocks).reshape((-1,) + (1,) * (len(dims) - 1 - dim))
    return level


def bell_draw(key, extent, scale, limit, cuts=(), held_as=jnp.bfloat16):
    values = jax.random.normal(key, extent, jnp.float32) * scale
    if len(cuts) > 0:
        values = steps_of(key, extent, cuts, -0.22, 0.18) * values
    return jnp.clip(values, min=-limit, max=limit).astype(held_as)


def setup_inputs(seed: int = 0) -> dict:
    splits = jax.random.split(jax.random.key(seed), 5)
    residual = bell_draw(splits[0], (PANELS, TILES, TILE_H, TILE_W, COLS), 1.0, 6.0, ((0, 4), (1, 8)), jnp.float32)
    inverse = draw_inverse(jax.random.fold_in(splits[4], 71), 0)
    blend_weight = jnp.clip(1.0 + 0.18 * jax.random.normal(splits[2], (CELLS,), jnp.float32), 0.1, 1.9)
    seam_table = draw_seam_table(jax.random.fold_in(splits[4], 71), 0)
    return {"residual": residual, "inverse": inverse, "blend_weight": blend_weight, "seam_table": seam_table}


def edge_strip(values, edge_id):
    margin = INTERSECTION
    if edge_id == 0:
        return jnp.transpose(values[:, :margin], (1, 0, 2))
    if edge_id == 1:
        return values[:margin]
    if edge_id == 2:
        return jnp.transpose(values[:, ::-1][:, :margin], (1, 0, 2))
    return values[::-1][:margin]


def incoming(strips, seam_table, panel_id, edge_id):
    seam_entry = seam_table[panel_id, edge_id]
    neighbour = jnp.maximum(seam_entry[0], 0)
    facing = (edge_id + 2 + seam_entry[1]) % 4
    picked = strips[neighbour, facing]
    picked = jnp.where(seam_entry[2] > 0, picked[:, ::-1], picked)
    return jnp.where(seam_entry[0] >= 0, picked, jnp.zeros_like(picked))


def with_ghosts(values, ghost_sets):
    margin = INTERSECTION
    widened = [jnp.pad(band, ((0, 0), (margin, margin), (0, 0))) for band in ghost_sets]
    padded = jnp.pad(values, ((margin, margin), (margin, margin), (0, 0)))
    padded = padded.at[:, :margin].set(jnp.transpose(widened[0][::-1], (1, 0, 2)))
    padded = padded.at[:margin, :].set(widened[1][::-1])
    padded = padded.at[:, -margin:].set(jnp.transpose(widened[2], (1, 0, 2)))
    padded = padded.at[-margin:, :].set(widened[3])
    return padded


def ghost_bands(padded):
    margin = INTERSECTION
    interior = padded.shape[0] - 2 * margin
    western = jnp.transpose(padded[margin:margin + interior, :margin][:, ::-1], (1, 0, 2))
    southern = padded[:margin, margin:margin + interior][::-1]
    eastern = jnp.transpose(padded[margin:margin + interior, -margin:], (1, 0, 2))
    northern = padded[-margin:, margin:margin + interior]
    return [western, southern, eastern, northern]


def add_bands(values, ghost_sets):
    margin = INTERSECTION
    values = values.at[:, :margin].add(jnp.transpose(ghost_sets[0], (1, 0, 2)))
    values = values.at[:margin].add(ghost_sets[1])
    values = values.at[:, -margin:].add(jnp.transpose(ghost_sets[2][::-1], (1, 0, 2)))
    values = values.at[-margin:].add(ghost_sets[3][::-1])
    return values


def patches(padded, block_rows, block_cols):
    columns = padded.shape[-1]
    blocked = padded.reshape(block_rows + 2, SUB, block_cols + 2, SUB, columns)
    pieces = [blocked[row_shift:row_shift + block_rows, :, col_shift:col_shift + block_cols]
              for row_shift in range(3) for col_shift in range(3)]
    stacked = jnp.stack(pieces).reshape(3, 3, block_rows, SUB, block_cols, SUB, columns)
    stacked = jnp.transpose(stacked, (2, 4, 0, 3, 1, 5, 6))
    return stacked.reshape(block_rows, block_cols, 9 * SUB * SUB, columns)


def intersection_add(solved, block_rows, block_cols):
    columns = solved.shape[-1]
    shaped = solved.reshape(block_rows, block_cols, 3, SUB, 3, SUB, columns)
    summed = jnp.zeros((block_rows + 2, SUB, block_cols + 2, SUB, columns), jnp.float32)
    for row_shift in range(3):
        for col_shift in range(3):
            block_part = jnp.transpose(shaped[:, :, row_shift, :, col_shift], (0, 2, 1, 3, 4))
            summed = summed.at[row_shift:row_shift + block_rows, :, col_shift:col_shift + block_cols].add(block_part)
    return summed.reshape((block_rows + 2) * SUB, (block_cols + 2) * SUB, columns)


def reference(residual, inverse, blend_weight, seam_table):
    margin = INTERSECTION
    tile_rows = residual.shape[1] // TILE_COLS
    height, tile_width, columns = residual.shape[2], residual.shape[3], residual.shape[4]
    panel_side = tile_width * TILE_COLS
    sub_rows, sub_cols = height // SUB, tile_width // SUB
    block_rows, block_cols = tile_rows * sub_rows, TILE_COLS * sub_cols
    cells = 9 * SUB * SUB
    panel_grid = residual.reshape(PANELS, tile_rows, TILE_COLS, height, tile_width, columns)
    panel_grid = jnp.transpose(panel_grid, (0, 1, 3, 2, 4, 5)).reshape(PANELS, panel_side, panel_side, columns)
    source = panel_grid.astype(jnp.bfloat16)
    strips = jnp.stack([jnp.stack([edge_strip(source[panel_id], edge_id) for edge_id in range(4)])
                        for panel_id in range(PANELS)])
    vectors = []
    for panel_id in range(PANELS):
        padded = with_ghosts(source[panel_id], [incoming(strips, seam_table, panel_id, edge_id) for edge_id in range(4)])
        local_patches = patches(padded, block_rows, block_cols)
        local_patches = local_patches.reshape(tile_rows, sub_rows, TILE_COLS, sub_cols, cells, columns)
        local_patches = jnp.transpose(local_patches, (0, 2, 1, 3, 4, 5))
        vectors.append(local_patches.reshape(tile_rows * TILE_COLS, sub_rows * sub_cols, cells, columns))
    vectors = jnp.stack(vectors)
    tile_count = PANELS * tile_rows * TILE_COLS

    def solve(operands):
        return jnp.einsum("noi,nir->nor", operands[0].astype(jnp.float32), operands[1].astype(jnp.float32))

    solved = lax.map(solve, (inverse.reshape((tile_count,) + inverse.shape[2:]),
                             vectors.reshape((tile_count,) + vectors.shape[2:])))
    solved = solved * blend_weight[None, None, :, None]
    solved = solved.reshape(PANELS, tile_rows, TILE_COLS, sub_rows, sub_cols, cells, columns)
    solved = jnp.transpose(solved, (0, 1, 3, 2, 4, 5, 6)).reshape(PANELS, block_rows, block_cols, cells, columns)
    spread = jnp.stack([intersection_add(solved[panel_id], block_rows, block_cols) for panel_id in range(PANELS)])
    ghost_sets = jnp.stack([jnp.stack(ghost_bands(spread[panel_id])) for panel_id in range(PANELS)])
    interior = spread[:, margin:margin + panel_side, margin:margin + panel_side]
    folded = jnp.stack([add_bands(interior[panel_id],
                                  [incoming(ghost_sets, seam_table, panel_id, edge_id) for edge_id in range(4)])
                        for panel_id in range(PANELS)])
    folded = folded.reshape(PANELS, tile_rows, height, TILE_COLS, tile_width, columns)
    return jnp.transpose(folded, (0, 1, 3, 2, 4, 5)).reshape(residual.shape)
```

```python
import functools

import jax
import jax.numpy as jnp
from jax import lax
from jax.experimental import pallas as pl
from jax.experimental.pallas import tpu as pltpu
from jax.sharding import PartitionSpec as P

TILE_ROWS = 2
SUB = 8
CELL = SUB * SUB
MESH = pl.DeviceIdType.MESH
SLOTS = 4
UNROLLED = 8
BF = jnp.bfloat16
F32 = jnp.float32


def repeat(count, body):
    if count <= UNROLLED:
        for step in range(count):
            body(step)
    else:
        pl.loop(0, count)(body)


def wrapped(index, size):
    return lax.rem(index + size, size)


def pick(options, index):
    out = options[-1]
    for place in range(len(options) - 2, -1, -1):
        out = jnp.where(index == place, options[place], out)
    return out


def kernel(
    panels, tiles, sub_rows,
    seam, residual, inverse, blend, out,
    held, shared, window_out, window_in, ghost_out, ghost_in, part_out, part_in,
    ext, spread, weight, inv_sem,
    tile_send, tile_recv, win_send, win_recv, gho_send, gho_recv, par_send, par_recv,
):
    cols = tiles // TILE_ROWS
    side = cols
    depth = sub_rows + 2
    panel, tile = lax.axis_index("panel"), lax.axis_index("tile")
    row, col = lax.div(tile, cols), lax.rem(tile, cols)

    def on_edge(edge, at_row, at_col):
        return pick([at_col == 0, at_row == 0, at_col == cols - 1, at_row == TILE_ROWS - 1], edge)

    def live_edge(of_panel, at_row, at_col):
        edge, found = jnp.int32(0), jnp.int32(0)
        for e in range(4):
            here = on_edge(e, at_row, at_col) & (seam[of_panel, e, 0] >= 0)
            edge = jnp.where(here, e, edge)
            found = jnp.where(here, 1, found)
        return edge, found

    def window_start(edge):
        return jnp.where(lax.rem(edge, 2) == 0, row * sub_rows, col) - 1

    def window_length(edge):
        return jnp.where(lax.rem(edge, 2) == 0, depth, 3)

    barrier = pltpu.get_barrier_semaphore()

    def greet_tile(step):
        pl.semaphore_signal(
            barrier, inc=1, device_id=(panel, wrapped(tile + step + 1, tiles)), device_id_type=MESH
        )

    repeat(tiles - 1, greet_tile)
    for off in range(1, panels):
        pl.semaphore_signal(
            barrier, inc=1, device_id=(wrapped(panel + off, panels), tile), device_id_type=MESH
        )

    def load_inverse(n):
        slot = lax.rem(n, SLOTS) if not isinstance(n, int) else n % SLOTS
        return pltpu.make_async_copy(inverse.at[n], held.at[slot], inv_sem.at[slot])

    for n in range(min(sub_rows, SLOTS)):
        load_inverse(n).start()

    def own_blocks(j):
        block = residual[pl.ds(j * SUB, SUB)].reshape(CELL, -1)
        shared[tile, j] = block.astype(BF)

    repeat(sub_rows, own_blocks)
    window_in[panel] = jnp.zeros(window_in.shape[1:], BF)
    ghost_in[panel] = jnp.zeros(ghost_in.shape[1:], BF)
    pl.semaphore_wait(barrier, tiles - 1 + panels - 1)

    def tile_copy(step, slot, target):
        return pltpu.make_async_remote_copy(
            src_ref=shared.at[slot], dst_ref=shared.at[slot],
            send_sem=tile_send.at[step], recv_sem=tile_recv.at[slot],
            device_id=(panel, target), device_id_type=MESH,
        )

    repeat(tiles - 1, lambda s: tile_copy(s, tile, wrapped(tile + s + 1, tiles)).start())

    lanes = residual.shape[-1]
    weight[...] = jnp.transpose(jnp.broadcast_to(blend[...], (lanes, blend.shape[1])))
    edge, found = live_edge(panel, row, col)
    neighbour = jnp.maximum(seam[panel, edge, 0], 0)
    facing = lax.rem(edge + 2 + seam[panel, edge, 1], 4)
    reverse = seam[panel, edge, 2]

    def source_cell(ghost):
        i, j = lax.shift_right_logical(ghost, 3), ghost & (SUB - 1)
        d = pick([SUB - 1 - j, SUB - 1 - i, j, i], edge)
        s = jnp.where(lax.rem(edge, 2) == 0, i, j)
        s = jnp.where(reverse > 0, SUB - 1 - s, s)
        across = jnp.where(facing >= 2, SUB - 1 - d, d)
        return jnp.where(lax.rem(facing, 2) == 0, s * SUB + across, across * SUB + s)

    shape = (CELL, CELL)
    first, second = lax.broadcasted_iota(jnp.int32, shape, 0), lax.broadcasted_iota(jnp.int32, shape, 1)
    turn = jnp.where((source_cell(first) == second) & (found > 0), 1.0, 0.0).astype(BF)
    turn_back = jnp.where((source_cell(second) == first) & (found > 0), 1.0, 0.0).astype(BF)

    def tile_arrival(step):
        source = wrapped(tile - step - 1, tiles)
        tile_copy(step, source, source).wait_recv()

    repeat(tiles - 1, tile_arrival)

    def window_copy(off, slot, target):
        return pltpu.make_async_remote_copy(
            src_ref=window_out.at[off - 1], dst_ref=window_in.at[slot],
            send_sem=win_send.at[off - 1], recv_sem=win_recv.at[slot],
            device_id=(target, tile), device_id_type=MESH,
        )

    for off in range(1, panels):
        other = wrapped(panel + off, panels)
        its_edge, its_found = live_edge(other, row, col)
        ours = (its_found > 0) & (seam[other, its_edge, 0] == panel)
        my_edge = lax.rem(its_edge + 2 + seam[other, its_edge, 1], 4)
        flip = seam[other, its_edge, 2]
        start, length = window_start(its_edge), window_length(its_edge)

        def fill(k, off=off, ours=ours, my_edge=my_edge, flip=flip, start=start, length=length):
            b = start + k
            good = ours & (b >= 0) & (b < side) & (k < length)
            b = jnp.where(flip > 0, side - 1 - b, b)
            b = jnp.clip(b, 0, side - 1)
            at_row = pick([b, 0, b, side - 1], my_edge)
            at_col = pick([0, b, cols - 1, b], my_edge)
            block = shared[lax.div(at_row, sub_rows) * cols + at_col, lax.rem(at_row, sub_rows)]
            window_out[off - 1, k] = jnp.where(good, block, jnp.zeros_like(block))

        repeat(depth, fill)
        window_copy(off, panel, other).start()

    def inner(ri):
        for ci in range(3):
            at_row, at_col = row * sub_rows + ri - 1, col + ci - 1
            inside = (at_row >= 0) & (at_row < side) & (at_col >= 0) & (at_col < cols)
            at_row, at_col = jnp.clip(at_row, 0, side - 1), jnp.clip(at_col, 0, cols - 1)
            block = shared[lax.div(at_row, sub_rows) * cols + at_col, lax.rem(at_row, sub_rows)]
            block = block.astype(F32)
            block = jnp.where(inside, block, jnp.zeros_like(block))
            ext[ri, :, ci] = block.reshape(SUB, SUB, lanes)

    repeat(depth, inner)

    for off in range(1, panels):
        source = wrapped(panel - off, panels)
        window_copy(off, source, source).wait_recv()

    def outer_side(k):
        block = jnp.dot(turn, window_in[neighbour, k], preferred_element_type=F32)
        block = block.reshape(SUB, SUB, lanes)
        for e, (ri, ci) in enumerate(((k, 0), (0, k), (k, 2), (depth - 1, k))):
            if e % 2 == 1 and not (isinstance(k, int) and k < 3):
                continue
            ext[ri, :, ci] += jnp.where(edge == e, block, jnp.zeros_like(block))

    for k in range(3):
        outer_side(k)
    if depth > 3:
        repeat_from = depth - 3
        repeat(repeat_from, lambda k: outer_side(jnp.int32(k) + 3 if isinstance(k, int) else k + 3))

    spread[...] = jnp.zeros_like(spread)

    def solve(n):
        load_inverse(n).wait()
        slot = n % SLOTS if isinstance(n, int) else lax.rem(n, SLOTS)
        patch = ext[pl.ds(n, 3)].reshape(9 * CELL, lanes).astype(BF)
        solved = jnp.dot(held[slot], patch, preferred_element_type=F32) * weight[...]
        spread[pl.ds(n, 3)] += solved.reshape(3, SUB, 3, SUB, lanes)
        if sub_rows > SLOTS:
            @pl.when(n + SLOTS < sub_rows)
            def _():
                load_inverse(n + SLOTS).start()

    repeat(sub_rows, solve)

    def ghost_copy(off, slot, target):
        return pltpu.make_async_remote_copy(
            src_ref=ghost_out, dst_ref=ghost_in.at[slot],
            send_sem=gho_send.at[off - 1], recv_sem=gho_recv.at[slot],
            device_id=(target, tile), device_id_type=MESH,
        )

    def ghost(k):
        even = lax.rem(edge, 2) == 0
        ri = jnp.where(even, k, jnp.where(edge == 1, 0, depth - 1))
        ci = jnp.where(even, edge, jnp.minimum(k, 2))
        raw = spread[ri, :, ci].reshape(CELL, lanes).astype(BF)
        ghost_out[k] = jnp.dot(turn_back, raw, preferred_element_type=F32).astype(BF)

    repeat(depth, ghost)
    for off in range(1, panels):
        ghost_copy(off, panel, wrapped(panel + off, panels)).start()
    for off in range(1, panels):
        source = wrapped(panel - off, panels)
        ghost_copy(off, source, source).wait_recv()

    def part(target, j):
        at_row, at_col = lax.div(target, cols), lax.rem(target, cols)
        ri, ci = (at_row - row) * sub_rows + j + 1, at_col - col + 1
        near = (ri >= 0) & (ri < depth) & (ci >= 0) & (ci < 3)
        block = spread[jnp.clip(ri, 0, depth - 1), :, jnp.clip(ci, 0, 2)].reshape(CELL, lanes)
        block = jnp.where(near, block, jnp.zeros_like(block))
        its_edge, its_found = live_edge(panel, at_row, at_col)
        other = jnp.maximum(seam[panel, its_edge, 0], 0)
        far_edge = lax.rem(its_edge + 2 + seam[panel, its_edge, 1], 4)
        even = lax.rem(its_edge, 2) == 0
        b = jnp.where(even, at_row * sub_rows + j, at_col)
        good = (its_found > 0) & on_edge(far_edge, row, col)
        good = good & (even | (j == jnp.where(its_edge == 1, 0, sub_rows - 1)))
        b = jnp.where(seam[panel, its_edge, 2] > 0, side - 1 - b, b)
        k = b - window_start(far_edge)
        good = good & (k >= 0) & (k < window_length(far_edge))
        seam_block = ghost_in[other, jnp.clip(k, 0, depth - 1)].astype(F32)
        return block + jnp.where(good, seam_block, jnp.zeros_like(seam_block))

    def part_copy(step, slot, target):
        return pltpu.make_async_remote_copy(
            src_ref=part_out.at[step], dst_ref=part_in.at[slot],
            send_sem=par_send.at[step], recv_sem=par_recv.at[slot],
            device_id=(panel, target), device_id_type=MESH,
        )

    def send_part(step):
        target = wrapped(tile + step + 1, tiles)

        def one(j):
            part_out[step, j] = part(target, j).astype(BF)

        repeat(sub_rows, one)
        part_copy(step, tile, target).start()

    repeat(tiles - 1, send_part)

    def own_part(j):
        out[pl.ds(j * SUB, SUB)] = part(tile, j).reshape(SUB, SUB, lanes)

    repeat(sub_rows, own_part)

    def take_part(step):
        source = wrapped(tile - step - 1, tiles)
        part_copy(step, source, source).wait_recv()

        def one(j):
            here = pl.ds(j * SUB, SUB)
            out[here] += part_in[source, j].astype(F32).reshape(SUB, SUB, lanes)

        repeat(sub_rows, one)

    repeat(tiles - 1, take_part)

    def sent(step):
        tile_copy(step, tile, wrapped(tile + step + 1, tiles)).wait_send()
        part_copy(step, tile, wrapped(tile + step + 1, tiles)).wait_send()

    repeat(tiles - 1, sent)
    for off in range(1, panels):
        window_copy(off, panel, wrapped(panel + off, panels)).wait_send()
        ghost_copy(off, panel, wrapped(panel + off, panels)).wait_send()


def local(panels, tiles, residual, inverse, blend_weight, seam_table):
    height, width, lanes = residual.shape[2:]
    sub_rows = height // SUB
    depth = sub_rows + 2
    cells = blend_weight.shape[0]
    vmem = pl.BlockSpec(memory_space=pltpu.VMEM)
    sem = pltpu.SemaphoreType.DMA
    block = (CELL, lanes)
    out = pl.pallas_call(
        functools.partial(kernel, panels, tiles, sub_rows),
        out_shape=jax.ShapeDtypeStruct((height, width, lanes), F32),
        in_specs=[
            pl.BlockSpec(memory_space=pltpu.SMEM), vmem, pl.BlockSpec(memory_space=pl.ANY), vmem,
        ],
        out_specs=vmem,
        scratch_shapes=[
            pltpu.VMEM((min(sub_rows, SLOTS), cells, cells), BF),
            pltpu.VMEM((tiles, sub_rows) + block, BF),
            pltpu.VMEM((panels - 1, depth) + block, BF),
            pltpu.VMEM((panels, depth) + block, BF),
            pltpu.VMEM((depth,) + block, BF),
            pltpu.VMEM((panels, depth) + block, BF),
            pltpu.VMEM((tiles - 1, sub_rows) + block, BF),
            pltpu.VMEM((tiles, sub_rows) + block, BF),
            pltpu.VMEM((depth, SUB, 3, SUB, lanes), F32),
            pltpu.VMEM((depth, SUB, 3, SUB, lanes), F32),
            pltpu.VMEM((cells, lanes), F32),
            sem((min(sub_rows, SLOTS),)),
            sem((tiles - 1,)), sem((tiles,)),
            sem((panels - 1,)), sem((panels,)),
            sem((panels - 1,)), sem((panels,)),
            sem((tiles - 1,)), sem((tiles,)),
        ],
        compiler_params=pltpu.CompilerParams(
            collective_id=0, has_side_effects=True, vmem_limit_bytes=67043328
        ),
    )(seam_table, residual[0, 0], inverse[0, 0], blend_weight[None])
    return out[None, None]


def solution(mesh):
    spec = P("panel", "tile", None, None, None)
    sizes = dict(mesh.shape)
    return jax.shard_map(
        functools.partial(local, sizes["panel"], sizes["tile"]),
        mesh=mesh,
        in_specs=(spec, spec, P(), P()),
        out_specs=spec,
        check_vma=False,
    )
```

```python
import functools

import jax
import jax.numpy as jnp
from jax import lax
from jax.experimental import pallas as pl
from jax.experimental.pallas import tpu as pltpu
from jax.sharding import PartitionSpec as P

TILE_ROWS = 2
SUB = 8
CELL = SUB * SUB
MESH = pl.DeviceIdType.MESH
SLOTS = 4
UNROLLED = 8
BF = jnp.bfloat16
F32 = jnp.float32


def repeat(count, body):
    if count <= UNROLLED:
        for step in range(count):
            body(step)
    else:
        pl.loop(0, count)(body)


def wrapped(index, size):
    return lax.rem(index + size, size)


def pick(options, index):
    out = options[-1]
    for place in range(len(options) - 2, -1, -1):
        out = jnp.where(index == place, options[place], out)
    return out


def kernel(
    panels, tiles, sub_rows,
    seam_in, residual, inverse, blend, out,
    held, shared, window_out, window_in, ghost_out, ghost_in, part_out, part_in,
    ext, spread, weight, seam, inv_sem, seam_sem,
    tile_send, tile_recv, win_send, win_recv, gho_send, gho_recv, par_send, par_recv,
):
    cols = tiles // TILE_ROWS
    side = cols
    depth = sub_rows + 2
    panel, tile = lax.axis_index("panel"), lax.axis_index("tile")
    row, col = lax.div(tile, cols), lax.rem(tile, cols)

    seam_copy = pltpu.make_async_copy(seam_in, seam, seam_sem.at[0])
    seam_copy.start()
    shift = jnp.where(row == 0, 1, 0)
    span = sub_rows + 1
    wide = max(3, span)

    def on_edge(edge, at_row, at_col):
        return pick([at_col == 0, at_row == 0, at_col == cols - 1, at_row == TILE_ROWS - 1], edge)

    def live_edge(of_panel, at_row, at_col):
        across = seam[of_panel, 0, 0] >= 0
        edge = jnp.where(across, jnp.where(at_col == 0, 0, 2), jnp.where(at_row == 0, 1, 3))
        return edge, on_edge(edge, at_row, at_col)

    def window_start(edge):
        return jnp.where(lax.rem(edge, 2) == 0, row * sub_rows - 1 + shift, col - 1)

    def window_length(edge):
        return jnp.where(lax.rem(edge, 2) == 0, span, 3)

    def planned(count, work):
        if count > UNROLLED:
            return work
        ready = [work(k) for k in range(count)]
        return lambda k: ready[k]

    barrier = pltpu.get_barrier_semaphore()

    def greet_tile(step):
        pl.semaphore_signal(
            barrier, inc=1, device_id=(panel, wrapped(tile + step + 1, tiles)), device_id_type=MESH
        )

    repeat(tiles - 1, greet_tile)
    for off in range(1, panels):
        pl.semaphore_signal(
            barrier, inc=1, device_id=(wrapped(panel + off, panels), tile), device_id_type=MESH
        )

    def load_inverse(n):
        slot = lax.rem(n, SLOTS) if not isinstance(n, int) else n % SLOTS
        return pltpu.make_async_copy(inverse.at[n], held.at[slot], inv_sem.at[slot])

    for n in range(min(sub_rows, SLOTS)):
        load_inverse(n).start()

    def own_blocks(j):
        block = residual[pl.ds(j * SUB, SUB)].reshape(CELL, -1)
        shared[tile * sub_rows + j] = block.astype(BF)
        shared[tiles * sub_rows + j] = jnp.zeros(block.shape, BF)

    repeat(sub_rows, own_blocks)
    window_in[panel] = jnp.zeros(window_in.shape[1:], BF)
    ghost_in[pl.ds(panel * wide, wide)] = jnp.zeros((wide,) + ghost_in.shape[1:], BF)
    spread[...] = jnp.zeros_like(spread)
    pl.semaphore_wait(barrier, tiles - 1 + panels - 1)

    def tile_copy(step, slot, target):
        return pltpu.make_async_remote_copy(
            src_ref=shared.at[pl.ds(slot * sub_rows, sub_rows)],
            dst_ref=shared.at[pl.ds(slot * sub_rows, sub_rows)],
            send_sem=tile_send.at[step], recv_sem=tile_recv.at[slot],
            device_id=(panel, target), device_id_type=MESH,
        )

    repeat(tiles - 1, lambda s: tile_copy(s, tile, wrapped(tile + s + 1, tiles)).start())

    lanes = residual.shape[-1]
    weight[...] = jnp.transpose(jnp.broadcast_to(blend[...].reshape(1, -1), (lanes, blend.shape[0])))
    seam_copy.wait()
    edge, found = live_edge(panel, row, col)
    neighbour = jnp.maximum(seam[panel, edge, 0], 0)
    facing = lax.rem(edge + 2 + seam[panel, edge, 1], 4)
    reverse = seam[panel, edge, 2]

    def source_cell(ghost):
        i, j = lax.shift_right_logical(ghost, 3), ghost & (SUB - 1)
        d = pick([SUB - 1 - j, SUB - 1 - i, j, i], edge)
        s = jnp.where(lax.rem(edge, 2) == 0, i, j)
        s = jnp.where(reverse > 0, SUB - 1 - s, s)
        across = jnp.where(facing >= 2, SUB - 1 - d, d)
        return jnp.where(lax.rem(facing, 2) == 0, s * SUB + across, across * SUB + s)

    shape = (CELL, CELL)
    first, second = lax.broadcasted_iota(jnp.int32, shape, 0), lax.broadcasted_iota(jnp.int32, shape, 1)
    turn = jnp.where((source_cell(first) == second) & found, 1.0, 0.0).astype(BF)
    turn_back = jnp.where((source_cell(second) == first) & found, 1.0, 0.0).astype(BF)

    def plan_window(off):
        other = wrapped(panel + off, panels)
        its_edge, its_found = live_edge(other, row, col)
        ours = its_found & (seam[other, its_edge, 0] == panel)
        my_edge = lax.rem(its_edge + 2 + seam[other, its_edge, 1], 4)
        flip = seam[other, its_edge, 2]
        start, length = window_start(its_edge), window_length(its_edge)

        def place(k):
            b = start + k
            good = ours & (b >= 0) & (b < side) & (k < length)
            b = jnp.where(flip > 0, side - 1 - b, b)
            at_row = pick([b, 0, b, side - 1], my_edge)
            at_col = pick([0, b, cols - 1, b], my_edge)
            block = (lax.div(at_row, sub_rows) * cols + at_col) * sub_rows + lax.rem(at_row, sub_rows)
            return jnp.where(good, block, tiles * sub_rows)

        return planned(wide, place)

    window_places = [plan_window(off) for off in range(1, panels)]

    def plan_inner(ri):
        places = []
        for ci in range(3):
            at_row, at_col = row * sub_rows + ri - 1, col + ci - 1
            inside = (at_row >= 0) & (at_row < side) & (at_col >= 0) & (at_col < cols)
            at_row = jnp.clip(at_row, 0, side - 1)
            block = (lax.div(at_row, sub_rows) * cols + at_col) * sub_rows + lax.rem(at_row, sub_rows)
            places.append(jnp.where(inside, block, tiles * sub_rows))
        return places

    inner_places = planned(depth, plan_inner)

    low = jnp.where(seam[panel, 0, 0] >= 0, 0, 1)
    seams = []
    for own in (low, low + 2):
        far_edge = lax.rem(own + 2 + seam[panel, own, 1], 4)
        far_start = window_start(far_edge)
        far_end = jnp.where(on_edge(far_edge, row, col), far_start + window_length(far_edge), -1)
        seams.append((seam[panel, own, 0], seam[panel, own, 2], far_start, far_end))

    def plan_part(target):
        at_row, at_col = lax.div(target, cols), lax.rem(target, cols)
        its_edge, its_found = live_edge(panel, at_row, at_col)
        other, flip, far_start, far_end = [
            jnp.where(its_edge < 2, lower, upper) for lower, upper in zip(*seams)
        ]

        def place(j):
            ri, ci = (at_row - row) * sub_rows + j + 1, at_col - col + 1
            near = (ri >= 0) & (ri < depth) & (ci >= 0) & (ci < 3)
            b = jnp.where(low == 0, at_row * sub_rows + j, at_col)
            good = its_found & ((low == 0) | (j == jnp.where(its_edge == 1, 0, sub_rows - 1)))
            b = jnp.where(flip > 0, side - 1 - b, b)
            good = good & (b >= far_start) & (b < far_end)
            return (
                jnp.where(near, ri, depth), jnp.where(near, ci, 0),
                jnp.where(good, other * wide + b - far_start, panel * wide),
            )

        return planned(sub_rows, place)

    part_places = planned(tiles, lambda step: plan_part(wrapped(tile + step, tiles)))

    def tile_arrival(step):
        source = wrapped(tile - step - 1, tiles)
        tile_copy(step, source, source).wait_recv()

    repeat(tiles - 1, tile_arrival)

    def window_copy(off, slot, target):
        return pltpu.make_async_remote_copy(
            src_ref=window_out.at[off - 1], dst_ref=window_in.at[slot],
            send_sem=win_send.at[off - 1], recv_sem=win_recv.at[slot],
            device_id=(target, tile), device_id_type=MESH,
        )

    for off in range(1, panels):
        def fill(k, off=off):
            window_out[off - 1, k] = shared[window_places[off - 1](k)]

        repeat(wide, fill)
        window_copy(off, panel, wrapped(panel + off, panels)).start()

    def inner(ri):
        for ci, place in enumerate(inner_places(ri)):
            ext[ri, :, ci] = shared[place].astype(F32).reshape(SUB, SUB, lanes)

    repeat(depth, inner)

    for off in range(1, panels):
        source = wrapped(panel - off, panels)
        window_copy(off, source, source).wait_recv()

    def outer_side(k):
        block = jnp.dot(turn, window_in[neighbour, k], preferred_element_type=F32)
        block = block.reshape(SUB, SUB, lanes)
        for e, (ri, ci) in enumerate(((k + shift, 0), (0, k), (k + shift, 2), (depth - 1, k))):
            if isinstance(k, int) and k < (3 if e % 2 else span):
                ext[ri, :, ci] += jnp.where(edge == e, block, jnp.zeros_like(block))
            elif not isinstance(k, int) and e % 2 == 0:
                ext[ri, :, ci] += jnp.where(edge == e, block, jnp.zeros_like(block))

    for k in range(3):
        outer_side(k)
    if span > 3:
        repeat(span - 3, lambda k: outer_side(jnp.int32(3) + k))

    def solve(n):
        load_inverse(n).wait()
        slot = n % SLOTS if isinstance(n, int) else lax.rem(n, SLOTS)
        patch = ext[pl.ds(n, 3)].reshape(9 * CELL, lanes).astype(BF)
        solved = jnp.dot(held[slot], patch, preferred_element_type=F32) * weight[...]
        spread[pl.ds(n, 3)] += solved.reshape(3, SUB, 3, SUB, lanes)
        if sub_rows > SLOTS:
            @pl.when(n + SLOTS < sub_rows)
            def _():
                load_inverse(n + SLOTS).start()

    repeat(sub_rows, solve)

    def ghost_copy(off, slot, target):
        return pltpu.make_async_remote_copy(
            src_ref=ghost_out, dst_ref=ghost_in.at[pl.ds(slot * wide, wide)],
            send_sem=gho_send.at[off - 1], recv_sem=gho_recv.at[slot],
            device_id=(target, tile), device_id_type=MESH,
        )

    def ghost(k):
        even = lax.rem(edge, 2) == 0
        ri = jnp.where(even, jnp.minimum(k + shift, depth - 1), jnp.where(edge == 1, 0, depth - 1))
        ci = jnp.where(even, edge, jnp.minimum(k, 2))
        raw = spread[ri, :, ci].reshape(CELL, lanes).astype(BF)
        ghost_out[k] = jnp.dot(turn_back, raw, preferred_element_type=F32).astype(BF)

    repeat(wide, ghost)
    for off in range(1, panels):
        ghost_copy(off, panel, wrapped(panel + off, panels)).start()
    for off in range(1, panels):
        source = wrapped(panel - off, panels)
        ghost_copy(off, source, source).wait_recv()

    def part(step, j):
        ri, ci, place = part_places(step)(j)
        return spread[ri, :, ci].reshape(CELL, lanes) + ghost_in[place].astype(F32)

    def part_copy(step, slot, target):
        return pltpu.make_async_remote_copy(
            src_ref=part_out.at[step], dst_ref=part_in.at[slot],
            send_sem=par_send.at[step], recv_sem=par_recv.at[slot],
            device_id=(panel, target), device_id_type=MESH,
        )

    def send_part(step):
        target = wrapped(tile + step + 1, tiles)

        def one(j):
            part_out[step, j] = part(step + 1, j).astype(BF)

        repeat(sub_rows, one)
        part_copy(step, tile, target).start()

    repeat(tiles - 1, send_part)

    def own_part(j):
        out[pl.ds(j * SUB, SUB)] = part(0, j).reshape(SUB, SUB, lanes)

    repeat(sub_rows, own_part)

    def take_part(step):
        source = wrapped(tile - step - 1, tiles)
        part_copy(step, source, source).wait_recv()

        def one(j):
            here = pl.ds(j * SUB, SUB)
            out[here] += part_in[source, j].astype(F32).reshape(SUB, SUB, lanes)

        repeat(sub_rows, one)

    repeat(tiles - 1, take_part)

    def sent(step):
        tile_copy(step, tile, wrapped(tile + step + 1, tiles)).wait_send()
        part_copy(step, tile, wrapped(tile + step + 1, tiles)).wait_send()

    repeat(tiles - 1, sent)
    for off in range(1, panels):
        window_copy(off, panel, wrapped(panel + off, panels)).wait_send()
        ghost_copy(off, panel, wrapped(panel + off, panels)).wait_send()


def local(panels, tiles, residual, inverse, blend_weight, seam_table):
    height, width, lanes = residual.shape[2:]
    sub_rows = height // SUB
    depth = sub_rows + 2
    wide = max(3, sub_rows + 1)
    cells = blend_weight.shape[0]
    vmem = pl.BlockSpec(memory_space=pltpu.VMEM)
    sem = pltpu.SemaphoreType.DMA
    block = (CELL, lanes)
    out = pl.pallas_call(
        functools.partial(kernel, panels, tiles, sub_rows),
        out_shape=jax.ShapeDtypeStruct((height, width, lanes), F32),
        in_specs=[
            pl.BlockSpec(memory_space=pl.ANY), vmem, pl.BlockSpec(memory_space=pl.ANY), vmem,
        ],
        out_specs=vmem,
        scratch_shapes=[
            pltpu.VMEM((min(sub_rows, SLOTS), cells, cells), BF),
            pltpu.VMEM(((tiles + 1) * sub_rows,) + block, BF),
            pltpu.VMEM((panels - 1, wide) + block, BF),
            pltpu.VMEM((panels, wide) + block, BF),
            pltpu.VMEM((wide,) + block, BF),
            pltpu.VMEM((panels * wide,) + block, BF),
            pltpu.VMEM((tiles - 1, sub_rows) + block, BF),
            pltpu.VMEM((tiles, sub_rows) + block, BF),
            pltpu.VMEM((depth, SUB, 3, SUB, lanes), F32),
            pltpu.VMEM((depth + 1, SUB, 3, SUB, lanes), F32),
            pltpu.VMEM((cells, lanes), F32),
            pltpu.SMEM(seam_table.shape, jnp.int32),
            sem((min(sub_rows, SLOTS),)), sem((1,)),
            sem((tiles - 1,)), sem((tiles,)),
            sem((panels - 1,)), sem((panels,)),
            sem((panels - 1,)), sem((panels,)),
            sem((tiles - 1,)), sem((tiles,)),
        ],
        compiler_params=pltpu.CompilerParams(
            collective_id=0, has_side_effects=True, vmem_limit_bytes=67043328
        ),
    )(seam_table, residual[0, 0], inverse[0, 0], blend_weight)
    return out[None, None]


def solution(mesh):
    spec = P("panel", "tile", None, None, None)
    sizes = dict(mesh.shape)
    return jax.shard_map(
        functools.partial(local, sizes["panel"], sizes["tile"]),
        mesh=mesh,
        in_specs=(spec, spec, P(), P()),
        out_specs=spec,
        check_vma=False,
    )
```

```python
import functools

import jax
import jax.numpy as jnp
from jax import lax
from jax.experimental import pallas as pl
from jax.experimental.pallas import tpu as pltpu
from jax.sharding import PartitionSpec as P

TILE_ROWS = 2
SUB = 8
CELL = SUB * SUB
MESH = pl.DeviceIdType.MESH
SLOTS = 4
UNROLLED = 8
BF = jnp.bfloat16
F32 = jnp.float32


def repeat(count, body):
    if count <= UNROLLED:
        for step in range(count):
            body(step)
    else:
        pl.loop(0, count)(body)


def wrapped(index, size):
    return lax.rem(index + size, size)


def pick(options, index):
    out = options[-1]
    for place in range(len(options) - 2, -1, -1):
        out = jnp.where(index == place, options[place], out)
    return out


def kernel(
    panels, tiles, sub_rows,
    seam_in, residual, inverse, blend, out,
    held, shared, window_out, window_in, ghost_out, ghost_in, part_out, part_in,
    ext, spread, weight, seam, inv_sem, seam_sem,
    tile_send, tile_recv, win_send, win_recv, gho_send, gho_recv, par_send, par_recv,
):
    cols = tiles // TILE_ROWS
    side = cols
    depth = sub_rows + 2
    panel, tile = lax.axis_index("panel"), lax.axis_index("tile")
    row, col = lax.div(tile, cols), lax.rem(tile, cols)

    seam_copy = pltpu.make_async_copy(seam_in, seam, seam_sem.at[0])
    seam_copy.start()
    shift = jnp.where(row == 0, 1, 0)
    span = sub_rows + 1
    wide = max(3, span)

    def on_edge(edge, at_row, at_col):
        return pick([at_col == 0, at_row == 0, at_col == cols - 1, at_row == TILE_ROWS - 1], edge)

    def live_edge(of_panel, at_row, at_col):
        across = seam[0, of_panel, 0] >= 0
        edge = jnp.where(across, jnp.where(at_col == 0, 0, 2), jnp.where(at_row == 0, 1, 3))
        return edge, on_edge(edge, at_row, at_col)

    def window_start(edge):
        return jnp.where(lax.rem(edge, 2) == 0, row * sub_rows - 1 + shift, col - 1)

    def window_length(edge):
        return jnp.where(lax.rem(edge, 2) == 0, span, 3)

    def peer(step, way):
        return wrapped(tile + way * (step + 1), tiles)

    def planned(count, work):
        if count > UNROLLED:
            return work
        ready = [work(k) for k in range(count)]
        return lambda k: ready[k]

    barrier = pltpu.get_barrier_semaphore()

    def greet_tile(step):
        pl.semaphore_signal(
            barrier, inc=1, device_id=(panel, peer(step, 1)), device_id_type=MESH
        )

    repeat(tiles - 1, greet_tile)
    for off in range(1, panels):
        pl.semaphore_signal(
            barrier, inc=1, device_id=(wrapped(panel + off, panels), tile), device_id_type=MESH
        )

    def load_inverse(n):
        slot = lax.rem(n, SLOTS) if not isinstance(n, int) else n % SLOTS
        return pltpu.make_async_copy(inverse.at[n], held.at[slot], inv_sem.at[slot])

    for n in range(min(sub_rows, SLOTS)):
        load_inverse(n).start()

    def own_blocks(j):
        block = residual[pl.ds(j * SUB, SUB)].reshape(CELL, -1)
        shared[tile * sub_rows + j] = block.astype(BF)
        shared[tiles * sub_rows + j] = jnp.zeros(block.shape, BF)

    repeat(sub_rows, own_blocks)
    window_in[panel] = jnp.zeros(window_in.shape[1:], BF)
    ghost_in[pl.ds(panel * wide, wide)] = jnp.zeros((wide,) + ghost_in.shape[1:], BF)
    spread[...] = jnp.zeros_like(spread)
    pl.semaphore_wait(barrier, tiles - 1 + panels - 1)

    def tile_copy(step, slot, target):
        return pltpu.make_async_remote_copy(
            src_ref=shared.at[pl.ds(slot * sub_rows, sub_rows)],
            dst_ref=shared.at[pl.ds(slot * sub_rows, sub_rows)],
            send_sem=tile_send.at[step], recv_sem=tile_recv.at[slot],
            device_id=(panel, target), device_id_type=MESH,
        )

    repeat(tiles - 1, lambda s: tile_copy(s, tile, peer(s, 1)).start())

    lanes = residual.shape[-1]
    weight[...] = jnp.transpose(jnp.broadcast_to(blend[...].reshape(1, -1), (lanes, blend.shape[0])))
    seam_copy.wait()
    edge, found = live_edge(panel, row, col)
    neighbour = jnp.maximum(seam[0, panel, edge], 0)
    facing = lax.rem(edge + 2 + seam[1, panel, edge], 4)
    reverse = seam[2, panel, edge]

    def source_cell(ghost):
        i, j = lax.shift_right_logical(ghost, 3), ghost & (SUB - 1)
        d = pick([SUB - 1 - j, SUB - 1 - i, j, i], edge)
        s = jnp.where(lax.rem(edge, 2) == 0, i, j)
        s = jnp.where(reverse > 0, SUB - 1 - s, s)
        across = jnp.where(facing >= 2, SUB - 1 - d, d)
        return jnp.where(lax.rem(facing, 2) == 0, s * SUB + across, across * SUB + s)

    shape = (CELL, CELL)
    first, second = lax.broadcasted_iota(jnp.int32, shape, 0), lax.broadcasted_iota(jnp.int32, shape, 1)
    turn = jnp.where((source_cell(first) == second) & found, 1.0, 0.0).astype(BF)
    turn_back = jnp.where((source_cell(second) == first) & found, 1.0, 0.0).astype(BF)

    def plan_window(off):
        other = wrapped(panel + off, panels)
        its_edge, its_found = live_edge(other, row, col)
        ours = its_found & (seam[0, other, its_edge] == panel)
        my_edge = lax.rem(its_edge + 2 + seam[1, other, its_edge], 4)
        flip = seam[2, other, its_edge]
        start, length = window_start(its_edge), window_length(its_edge)

        def place(k):
            b = start + k
            good = ours & (b >= 0) & (b < side) & (k < length)
            b = jnp.where(flip > 0, side - 1 - b, b)
            at_row = pick([b, 0, b, side - 1], my_edge)
            at_col = pick([0, b, cols - 1, b], my_edge)
            block = (lax.div(at_row, sub_rows) * cols + at_col) * sub_rows + lax.rem(at_row, sub_rows)
            return jnp.where(good, block, tiles * sub_rows)

        return planned(wide, place)

    window_places = [plan_window(off) for off in range(1, panels)]

    def plan_inner(ri):
        places = []
        for ci in range(3):
            at_row, at_col = row * sub_rows + ri - 1, col + ci - 1
            inside = (at_row >= 0) & (at_row < side) & (at_col >= 0) & (at_col < cols)
            at_row = jnp.clip(at_row, 0, side - 1)
            block = (lax.div(at_row, sub_rows) * cols + at_col) * sub_rows + lax.rem(at_row, sub_rows)
            places.append(jnp.where(inside, block, tiles * sub_rows))
        return places

    inner_places = planned(depth, plan_inner)

    low = jnp.where(seam[0, panel, 0] >= 0, 0, 1)
    seams = []
    for own in (low, low + 2):
        far_edge = lax.rem(own + 2 + seam[1, panel, own], 4)
        far_start = window_start(far_edge)
        far_end = jnp.where(on_edge(far_edge, row, col), far_start + window_length(far_edge), -1)
        seams.append((seam[0, panel, own], seam[2, panel, own], far_start, far_end))

    def plan_part(target):
        at_row, at_col = lax.div(target, cols), lax.rem(target, cols)
        its_edge, its_found = live_edge(panel, at_row, at_col)
        other, flip, far_start, far_end = [
            jnp.where(its_edge < 2, lower, upper) for lower, upper in zip(*seams)
        ]

        def place(j):
            ri, ci = (at_row - row) * sub_rows + j + 1, at_col - col + 1
            near = (ri >= 0) & (ri < depth) & (ci >= 0) & (ci < 3)
            b = jnp.where(low == 0, at_row * sub_rows + j, at_col)
            good = its_found & ((low == 0) | (j == jnp.where(its_edge == 1, 0, sub_rows - 1)))
            b = jnp.where(flip > 0, side - 1 - b, b)
            good = good & (b >= far_start) & (b < far_end)
            return (
                jnp.where(near, ri, depth), jnp.where(near, ci, 0),
                jnp.where(good, other * wide + b - far_start, panel * wide),
            )

        return planned(sub_rows, place)

    part_places = planned(tiles, lambda step: plan_part(peer(step, 1)))

    def tile_arrival(step):
        source = peer(step, -1)
        tile_copy(step, source, source).wait_recv()

    repeat(tiles - 1, tile_arrival)

    def window_copy(off, slot, target):
        return pltpu.make_async_remote_copy(
            src_ref=window_out.at[off - 1], dst_ref=window_in.at[slot],
            send_sem=win_send.at[off - 1], recv_sem=win_recv.at[slot],
            device_id=(target, tile), device_id_type=MESH,
        )

    for off in range(1, panels):
        def fill(k, off=off):
            window_out[off - 1, k] = shared[window_places[off - 1](k)]

        repeat(wide, fill)
        window_copy(off, panel, wrapped(panel + off, panels)).start()

    def inner(ri):
        for ci, place in enumerate(inner_places(ri)):
            ext[ri, :, ci] = shared[place].astype(F32).reshape(SUB, SUB, lanes)

    repeat(depth, inner)

    for off in range(1, panels):
        source = wrapped(panel - off, panels)
        window_copy(off, source, source).wait_recv()

    def outer_side(k):
        block = jnp.dot(turn, window_in[neighbour, k], preferred_element_type=F32)
        block = block.reshape(SUB, SUB, lanes)
        for e, (ri, ci) in enumerate(((k + shift, 0), (0, k), (k + shift, 2), (depth - 1, k))):
            if isinstance(k, int) and k < (3 if e % 2 else span):
                ext[ri, :, ci] += jnp.where(edge == e, block, jnp.zeros_like(block))
            elif not isinstance(k, int) and e % 2 == 0:
                ext[ri, :, ci] += jnp.where(edge == e, block, jnp.zeros_like(block))

    for k in range(3):
        outer_side(k)
    if span > 3:
        repeat(span - 3, lambda k: outer_side(jnp.int32(3) + k))

    def solve(n):
        load_inverse(n).wait()
        slot = n % SLOTS if isinstance(n, int) else lax.rem(n, SLOTS)
        patch = ext[pl.ds(n, 3)].reshape(9 * CELL, lanes).astype(BF)
        solved = jnp.dot(held[slot], patch, preferred_element_type=F32) * weight[...]
        spread[pl.ds(n, 3)] += solved.reshape(3, SUB, 3, SUB, lanes)
        if sub_rows > SLOTS:
            @pl.when(n + SLOTS < sub_rows)
            def _():
                load_inverse(n + SLOTS).start()

    repeat(sub_rows, solve)

    def ghost_copy(off, slot, target):
        return pltpu.make_async_remote_copy(
            src_ref=ghost_out, dst_ref=ghost_in.at[pl.ds(slot * wide, wide)],
            send_sem=gho_send.at[off - 1], recv_sem=gho_recv.at[slot],
            device_id=(target, tile), device_id_type=MESH,
        )

    def ghost(k):
        even = lax.rem(edge, 2) == 0
        ri = jnp.where(even, jnp.minimum(k + shift, depth - 1), jnp.where(edge == 1, 0, depth - 1))
        ci = jnp.where(even, edge, jnp.minimum(k, 2))
        raw = spread[ri, :, ci].reshape(CELL, lanes).astype(BF)
        ghost_out[k] = jnp.dot(turn_back, raw, preferred_element_type=F32).astype(BF)

    repeat(wide, ghost)
    for off in range(1, panels):
        ghost_copy(off, panel, wrapped(panel + off, panels)).start()
    for off in range(1, panels):
        source = wrapped(panel - off, panels)
        ghost_copy(off, source, source).wait_recv()

    def part(step, j):
        ri, ci, place = part_places(step)(j)
        return spread[ri, :, ci].reshape(CELL, lanes) + ghost_in[place].astype(F32)

    def part_copy(step, slot, target):
        return pltpu.make_async_remote_copy(
            src_ref=part_out.at[step], dst_ref=part_in.at[slot],
            send_sem=par_send.at[step], recv_sem=par_recv.at[slot],
            device_id=(panel, target), device_id_type=MESH,
        )

    def send_part(step):
        target = peer(step, 1)

        def one(j):
            part_out[step, j] = part(step, j).astype(BF)

        repeat(sub_rows, one)
        part_copy(step, tile, target).start()

    repeat(tiles - 1, send_part)

    def own_part(j):
        out[pl.ds(j * SUB, SUB)] = part(tiles - 1, j).reshape(SUB, SUB, lanes)

    repeat(sub_rows, own_part)

    def take_part(step):
        source = peer(step, -1)
        part_copy(step, source, source).wait_recv()

        def one(j):
            here = pl.ds(j * SUB, SUB)
            out[here] += part_in[source, j].astype(F32).reshape(SUB, SUB, lanes)

        repeat(sub_rows, one)

    repeat(tiles - 1, take_part)

    def sent(step):
        tile_copy(step, tile, peer(step, 1)).wait_send()
        part_copy(step, tile, peer(step, 1)).wait_send()

    repeat(tiles - 1, sent)
    for off in range(1, panels):
        window_copy(off, panel, wrapped(panel + off, panels)).wait_send()
        ghost_copy(off, panel, wrapped(panel + off, panels)).wait_send()


def local(panels, tiles, residual, inverse, blend_weight, seam_table):
    height, width, lanes = residual.shape[2:]
    sub_rows = height // SUB
    depth = sub_rows + 2
    wide = max(3, sub_rows + 1)
    cells = blend_weight.shape[0]
    vmem = pl.BlockSpec(memory_space=pltpu.VMEM)
    sem = pltpu.SemaphoreType.DMA
    block = (CELL, lanes)
    fields = jnp.transpose(seam_table, (2, 0, 1))
    out = pl.pallas_call(
        functools.partial(kernel, panels, tiles, sub_rows),
        out_shape=jax.ShapeDtypeStruct((height, width, lanes), F32),
        in_specs=[
            pl.BlockSpec(memory_space=pl.ANY), vmem, pl.BlockSpec(memory_space=pl.ANY), vmem,
        ],
        out_specs=vmem,
        scratch_shapes=[
            pltpu.VMEM((min(sub_rows, SLOTS), cells, cells), BF),
            pltpu.VMEM(((tiles + 1) * sub_rows,) + block, BF),
            pltpu.VMEM((panels - 1, wide) + block, BF),
            pltpu.VMEM((panels, wide) + block, BF),
            pltpu.VMEM((wide,) + block, BF),
            pltpu.VMEM((panels * wide,) + block, BF),
            pltpu.VMEM((tiles - 1, sub_rows) + block, BF),
            pltpu.VMEM((tiles, sub_rows) + block, BF),
            pltpu.VMEM((depth, SUB, 3, SUB, lanes), F32),
            pltpu.VMEM((depth + 1, SUB, 3, SUB, lanes), F32),
            pltpu.VMEM((cells, lanes), F32),
            pltpu.SMEM(fields.shape, jnp.int32),
            sem((min(sub_rows, SLOTS),)), sem((1,)),
            sem((tiles - 1,)), sem((tiles,)),
            sem((panels - 1,)), sem((panels,)),
            sem((panels - 1,)), sem((panels,)),
            sem((tiles - 1,)), sem((tiles,)),
        ],
        compiler_params=pltpu.CompilerParams(
            collective_id=0, has_side_effects=True, vmem_limit_bytes=67043328
        ),
    )(fields, residual[0, 0], inverse[0, 0], blend_weight)
    return out[None, None]


def solution(mesh):
    spec = P("panel", "tile", None, None, None)
    sizes = dict(mesh.shape)
    return jax.shard_map(
        functools.partial(local, sizes["panel"], sizes["tile"]),
        mesh=mesh,
        in_specs=(spec, spec, P(), P()),
        out_specs=spec,
        check_vma=False,
    )
```

```python
import functools

import jax
import jax.numpy as jnp
from jax import lax
from jax.experimental import pallas as pl
from jax.experimental.pallas import tpu as pltpu
from jax.sharding import PartitionSpec as P

TILE_ROWS = 2
SUB = 8
CELL = SUB * SUB
MESH = pl.DeviceIdType.MESH
SLOTS = 4
UNROLLED = 8
BF = jnp.bfloat16
F32 = jnp.float32


def repeat(count, body):
    if count <= UNROLLED:
        for step in range(count):
            body(step)
    else:
        pl.loop(0, count)(body)


def wrapped(index, size):
    return lax.rem(index + size, size)


def pick(options, index):
    out = options[-1]
    for place in range(len(options) - 2, -1, -1):
        out = jnp.where(index == place, options[place], out)
    return out


def kernel(
    panels, tiles, sub_rows,
    seam_in, residual, inverse, blend, out,
    held, shared, window_out, window_in, ghost_out, ghost_in, part_out, part_in,
    ext, spread, weight, seam, inv_sem, seam_sem,
    tile_send, tile_recv, win_send, win_recv, gho_send, gho_recv, par_send, par_recv,
    rest_in, halo_out, halo_in, rest_send, rest_recv, halo_send, halo_recv,
):
    cols = tiles // TILE_ROWS
    side = cols
    depth = sub_rows + 2
    panel, tile = lax.axis_index("panel"), lax.axis_index("tile")
    row, col = lax.div(tile, cols), lax.rem(tile, cols)

    seam_copy = pltpu.make_async_copy(seam_in, seam, seam_sem.at[0])
    seam_copy.start()
    shift = jnp.where(row == 0, 1, 0)
    span = sub_rows + 1
    wide = max(3, span)

    def on_edge(edge, at_row, at_col):
        return pick([at_col == 0, at_row == 0, at_col == cols - 1, at_row == TILE_ROWS - 1], edge)

    def live_edge(of_panel, at_row, at_col):
        across = seam[0, of_panel, 0] >= 0
        edge = jnp.where(across, jnp.where(at_col == 0, 0, 2), jnp.where(at_row == 0, 1, 3))
        return edge, on_edge(edge, at_row, at_col)

    def window_start(edge):
        return jnp.where(lax.rem(edge, 2) == 0, row * sub_rows - 1 + shift, col - 1)

    def window_length(edge):
        return jnp.where(lax.rem(edge, 2) == 0, span, 3)

    def peer(step, way):
        return wrapped(tile + way * (step + 1), tiles)

    near_tiles = ((0, -1), (0, 1), (1, -1), (1, 0), (1, 1))

    def near(slot, action):
        other_row, away = near_tiles[slot]
        at_col = col + away
        target = jnp.where(row == 0, other_row, 1 - other_row) * cols + at_col

        @pl.when((at_col >= 0) & (at_col < cols))
        def _():
            action(target, at_col, near_tiles.index((other_row, -away)))

    def at_side(at_col):
        return (at_col == 0) | (at_col == cols - 1)

    def rim(at_row):
        return jnp.where(at_row == 0, 0, sub_rows - 1)

    def either(test, yes, no):
        pl.when(test)(yes)
        pl.when(jnp.logical_not(test))(no)

    def planned(count, work):
        if count > UNROLLED:
            return work
        ready = [work(k) for k in range(count)]
        return lambda k: ready[k]

    barrier = pltpu.get_barrier_semaphore()

    def greet_tile(step):
        pl.semaphore_signal(
            barrier, inc=1, device_id=(panel, peer(step, 1)), device_id_type=MESH
        )

    repeat(tiles - 1, greet_tile)
    for off in range(1, panels):
        pl.semaphore_signal(
            barrier, inc=1, device_id=(wrapped(panel + off, panels), tile), device_id_type=MESH
        )

    def load_inverse(n):
        slot = lax.rem(n, SLOTS) if not isinstance(n, int) else n % SLOTS
        return pltpu.make_async_copy(inverse.at[n], held.at[slot], inv_sem.at[slot])

    for n in range(min(sub_rows, SLOTS)):
        load_inverse(n).start()

    def own_blocks(j):
        block = residual[pl.ds(j * SUB, SUB)].reshape(CELL, -1)
        shared[tile * sub_rows + j] = block.astype(BF)
        shared[tiles * sub_rows + j] = jnp.zeros(block.shape, BF)

    repeat(sub_rows, own_blocks)
    window_in[panel] = jnp.zeros(window_in.shape[1:], BF)
    ghost_in[pl.ds(panel * wide, wide)] = jnp.zeros((wide,) + ghost_in.shape[1:], BF)
    spread[...] = jnp.zeros_like(spread)
    rest_in[rest_in.shape[0] - 1] = jnp.zeros(rest_in.shape[1:], BF)
    pl.semaphore_wait(barrier, tiles - 1 + panels - 1)

    def tile_copy(step, slot, target, whole):
        at = slot * sub_rows + (0 if whole else rim(lax.div(slot, cols)))
        here = pl.ds(at, sub_rows if whole else 1)
        return pltpu.make_async_remote_copy(
            src_ref=shared.at[here], dst_ref=shared.at[here],
            send_sem=tile_send.at[step], recv_sem=tile_recv.at[slot],
            device_id=(panel, target), device_id_type=MESH,
        )

    def send_tile(step):
        either(
            at_side(col),
            lambda: tile_copy(step, tile, peer(step, 1), True).start(),
            lambda: tile_copy(step, tile, peer(step, 1), False).start(),
        )

    repeat(tiles - 1, send_tile)

    def rest_copy(slot, target, there):
        here = pl.ds(tile * sub_rows + jnp.where(row == 0, 1, 0), sub_rows - 1)
        return pltpu.make_async_remote_copy(
            src_ref=shared.at[here], dst_ref=rest_in.at[there],
            send_sem=rest_send.at[slot], recv_sem=rest_recv.at[there],
            device_id=(panel, target), device_id_type=MESH,
        )

    def rests(sending, act):
        if sub_rows == 1:
            return
        for slot in range(len(near_tiles)):
            def action(target, at_col, there, slot=slot):
                @pl.when(jnp.logical_not(at_side(col if sending else at_col)))
                def _():
                    act(rest_copy(slot, target, there if sending else slot))

            near(slot, action)

    lanes = residual.shape[-1]
    weight[...] = jnp.transpose(jnp.broadcast_to(blend[...].reshape(1, -1), (lanes, blend.shape[0])))
    seam_copy.wait()
    edge, found = live_edge(panel, row, col)
    neighbour = jnp.maximum(seam[0, panel, edge], 0)
    facing = lax.rem(edge + 2 + seam[1, panel, edge], 4)
    reverse = seam[2, panel, edge]

    def source_cell(ghost):
        i, j = lax.shift_right_logical(ghost, 3), ghost & (SUB - 1)
        d = pick([SUB - 1 - j, SUB - 1 - i, j, i], edge)
        s = jnp.where(lax.rem(edge, 2) == 0, i, j)
        s = jnp.where(reverse > 0, SUB - 1 - s, s)
        across = jnp.where(facing >= 2, SUB - 1 - d, d)
        return jnp.where(lax.rem(facing, 2) == 0, s * SUB + across, across * SUB + s)

    shape = (CELL, CELL)
    first, second = lax.broadcasted_iota(jnp.int32, shape, 0), lax.broadcasted_iota(jnp.int32, shape, 1)
    turn = jnp.where((source_cell(first) == second) & found, 1.0, 0.0).astype(BF)
    turn_back = jnp.where((source_cell(second) == first) & found, 1.0, 0.0).astype(BF)

    def plan_window(off):
        other = wrapped(panel + off, panels)
        its_edge, its_found = live_edge(other, row, col)
        ours = its_found & (seam[0, other, its_edge] == panel)
        my_edge = lax.rem(its_edge + 2 + seam[1, other, its_edge], 4)
        flip = seam[2, other, its_edge]
        start, length = window_start(its_edge), window_length(its_edge)

        def place(k):
            b = start + k
            good = ours & (b >= 0) & (b < side) & (k < length)
            b = jnp.where(flip > 0, side - 1 - b, b)
            at_row = pick([b, 0, b, side - 1], my_edge)
            at_col = pick([0, b, cols - 1, b], my_edge)
            block = (lax.div(at_row, sub_rows) * cols + at_col) * sub_rows + lax.rem(at_row, sub_rows)
            return jnp.where(good, block, tiles * sub_rows)

        return planned(wide, place)

    window_places = [plan_window(off) for off in range(1, panels)]

    def plan_inner(ri):
        places = []
        for ci in range(3):
            at_row, at_col = row * sub_rows + ri - 1, col + ci - 1
            inside = (at_row >= 0) & (at_row < side) & (at_col >= 0) & (at_col < cols)
            at_row = jnp.clip(at_row, 0, side - 1)
            tile_row, sub = lax.div(at_row, sub_rows), lax.rem(at_row, sub_rows)
            block = (tile_row * cols + at_col) * sub_rows + sub
            away = tile_row != row
            apart = inside & jnp.logical_not(at_side(at_col)) & (sub != rim(tile_row))
            if ci == 1:
                apart = apart & away
            same_row = near_tiles.index((0, ci - 1)) if ci != 1 else 0
            slot = jnp.where(away, near_tiles.index((1, ci - 1)), same_row)
            rest = jnp.clip(sub - jnp.where(tile_row == 0, 1, 0), 0, max(sub_rows - 2, 0))
            places.append((
                jnp.where(inside & jnp.logical_not(apart), block, tiles * sub_rows),
                jnp.where(apart, slot, len(near_tiles)), jnp.where(apart, rest, 0),
            ))
        return places

    inner_places = planned(depth, plan_inner)

    low = jnp.where(seam[0, panel, 0] >= 0, 0, 1)
    seams = []
    for own in (low, low + 2):
        far_edge = lax.rem(own + 2 + seam[1, panel, own], 4)
        far_start = window_start(far_edge)
        far_end = jnp.where(on_edge(far_edge, row, col), far_start + window_length(far_edge), -1)
        seams.append((seam[0, panel, own], seam[2, panel, own], far_start, far_end))

    def plan_part(target):
        at_row, at_col = lax.div(target, cols), lax.rem(target, cols)
        its_edge, its_found = live_edge(panel, at_row, at_col)
        other, flip, far_start, far_end = [
            jnp.where(its_edge < 2, lower, upper) for lower, upper in zip(*seams)
        ]

        def place(j):
            b = jnp.where(low == 0, at_row * sub_rows + j, at_col)
            good = its_found & ((low == 0) | (j == rim(at_row)))
            b = jnp.where(flip > 0, side - 1 - b, b)
            good = good & (b >= far_start) & (b < far_end)
            return jnp.where(good, other * wide + b - far_start, panel * wide)

        return planned(sub_rows, place)

    part_places = planned(tiles, lambda step: plan_part(peer(step, 1)))

    def tile_arrival(step):
        source = peer(step, -1)
        either(
            at_side(lax.rem(source, cols)),
            lambda: tile_copy(step, source, source, True).wait_recv(),
            lambda: tile_copy(step, source, source, False).wait_recv(),
        )

    repeat(tiles - 1, tile_arrival)

    def window_copy(off, slot, target):
        return pltpu.make_async_remote_copy(
            src_ref=window_out.at[off - 1], dst_ref=window_in.at[slot],
            send_sem=win_send.at[off - 1], recv_sem=win_recv.at[slot],
            device_id=(target, tile), device_id_type=MESH,
        )

    for off in range(1, panels):
        def fill(k, off=off):
            window_out[off - 1, k] = shared[window_places[off - 1](k)]

        repeat(wide, fill)
        window_copy(off, panel, wrapped(panel + off, panels)).start()

    rests(True, lambda copy: copy.start())
    rests(False, lambda copy: copy.wait_recv())

    def inner(ri):
        for ci, (place, slot, rest) in enumerate(inner_places(ri)):
            block = shared[place].astype(F32)
            if sub_rows > 1:
                block = block + rest_in[slot, rest].astype(F32)
            ext[ri, :, ci] = block.reshape(SUB, SUB, lanes)

    repeat(depth, inner)

    for off in range(1, panels):
        source = wrapped(panel - off, panels)
        window_copy(off, source, source).wait_recv()

    def outer_side(k):
        block = jnp.dot(turn, window_in[neighbour, k], preferred_element_type=F32)
        block = block.reshape(SUB, SUB, lanes)
        for e, (ri, ci) in enumerate(((k + shift, 0), (0, k), (k + shift, 2), (depth - 1, k))):
            if isinstance(k, int) and k < (3 if e % 2 else span):
                ext[ri, :, ci] += jnp.where(edge == e, block, jnp.zeros_like(block))
            elif not isinstance(k, int) and e % 2 == 0:
                ext[ri, :, ci] += jnp.where(edge == e, block, jnp.zeros_like(block))

    for k in range(3):
        outer_side(k)
    if span > 3:
        repeat(span - 3, lambda k: outer_side(jnp.int32(3) + k))

    def solve(n):
        load_inverse(n).wait()
        slot = n % SLOTS if isinstance(n, int) else lax.rem(n, SLOTS)
        patch = ext[pl.ds(n, 3)].reshape(9 * CELL, lanes).astype(BF)
        solved = jnp.dot(held[slot], patch, preferred_element_type=F32) * weight[...]
        spread[pl.ds(n, 3)] += solved.reshape(3, SUB, 3, SUB, lanes)
        if sub_rows > SLOTS:
            @pl.when(n + SLOTS < sub_rows)
            def _():
                load_inverse(n + SLOTS).start()

    repeat(sub_rows, solve)

    def ghost_copy(off, slot, target):
        return pltpu.make_async_remote_copy(
            src_ref=ghost_out, dst_ref=ghost_in.at[pl.ds(slot * wide, wide)],
            send_sem=gho_send.at[off - 1], recv_sem=gho_recv.at[slot],
            device_id=(target, tile), device_id_type=MESH,
        )

    def ghost(k):
        even = lax.rem(edge, 2) == 0
        ri = jnp.where(even, jnp.minimum(k + shift, depth - 1), jnp.where(edge == 1, 0, depth - 1))
        ci = jnp.where(even, edge, jnp.minimum(k, 2))
        raw = spread[ri, :, ci].reshape(CELL, lanes).astype(BF)
        ghost_out[k] = jnp.dot(turn_back, raw, preferred_element_type=F32).astype(BF)

    repeat(wide, ghost)
    for off in range(1, panels):
        ghost_copy(off, panel, wrapped(panel + off, panels)).start()

    def halo_copy(slot, target, there):
        size = sub_rows if near_tiles[slot][0] == 0 else 1
        return pltpu.make_async_remote_copy(
            src_ref=halo_out.at[slot, pl.ds(0, size)], dst_ref=halo_in.at[there, pl.ds(0, size)],
            send_sem=halo_send.at[slot], recv_sem=halo_recv.at[there],
            device_id=(panel, target), device_id_type=MESH,
        )

    for slot, (other_row, away) in enumerate(near_tiles):
        def send_halo(target, at_col, there, slot=slot, other_row=other_row, away=away):
            def one(j):
                ri = jnp.where(row == 0, depth - 1, 0) if other_row else j + 1
                halo_out[slot, j] = spread[ri, :, away + 1].reshape(CELL, lanes).astype(BF)

            repeat(1 if other_row else sub_rows, one)
            halo_copy(slot, target, there).start()

        near(slot, send_halo)

    def own_part(j):
        out[pl.ds(j * SUB, SUB)] = spread[j + 1, :, 1]

    repeat(sub_rows, own_part)

    for off in range(1, panels):
        source = wrapped(panel - off, panels)
        ghost_copy(off, source, source).wait_recv()

    def part_copy(step, slot, target, whole):
        here = pl.ds(0, sub_rows) if whole else pl.ds(rim(lax.div(target, cols)), 1)
        return pltpu.make_async_remote_copy(
            src_ref=part_out.at[step, here], dst_ref=part_in.at[slot, here],
            send_sem=par_send.at[step], recv_sem=par_recv.at[slot],
            device_id=(panel, target), device_id_type=MESH,
        )

    def send_part(step):
        target = peer(step, 1)

        def one(j):
            part_out[step, j] = ghost_in[part_places(step)(j)]

        repeat(sub_rows, one)
        either(
            at_side(lax.rem(target, cols)),
            lambda: part_copy(step, tile, target, True).start(),
            lambda: part_copy(step, tile, target, False).start(),
        )

    repeat(tiles - 1, send_part)

    def add(j, block):
        out[pl.ds(j * SUB, SUB)] += block.astype(F32).reshape(SUB, SUB, lanes)

    repeat(sub_rows, lambda j: add(j, ghost_in[part_places(tiles - 1)(j)]))

    for slot, (other_row, _) in enumerate(near_tiles):
        def take_halo(target, at_col, there, slot=slot, other_row=other_row):
            halo_copy(slot, target, slot).wait_recv()
            if other_row:
                add(jnp.where(row == 0, sub_rows - 1, 0), halo_in[slot, 0])
            else:
                repeat(sub_rows, lambda j: add(j, halo_in[slot, j]))

        near(slot, take_halo)

    def take_part(step):
        source = peer(step, -1)

        def whole():
            part_copy(step, source, tile, True).wait_recv()
            repeat(sub_rows, lambda j: add(j, part_in[source, j]))

        def outermost():
            part_copy(step, source, tile, False).wait_recv()
            add(rim(row), part_in[source, rim(row)])

        either(at_side(col), whole, outermost)

    repeat(tiles - 1, take_part)

    def sent(step):
        target = peer(step, 1)
        either(
            at_side(col),
            lambda: tile_copy(step, tile, target, True).wait_send(),
            lambda: tile_copy(step, tile, target, False).wait_send(),
        )
        either(
            at_side(lax.rem(target, cols)),
            lambda: part_copy(step, tile, target, True).wait_send(),
            lambda: part_copy(step, tile, target, False).wait_send(),
        )

    repeat(tiles - 1, sent)
    rests(True, lambda copy: copy.wait_send())
    for slot in range(len(near_tiles)):
        near(slot, lambda target, at_col, there, slot=slot: halo_copy(slot, target, there).wait_send())
    for off in range(1, panels):
        window_copy(off, panel, wrapped(panel + off, panels)).wait_send()
        ghost_copy(off, panel, wrapped(panel + off, panels)).wait_send()


def local(panels, tiles, residual, inverse, blend_weight, seam_table):
    height, width, lanes = residual.shape[2:]
    sub_rows = height // SUB
    depth = sub_rows + 2
    wide = max(3, sub_rows + 1)
    cells = blend_weight.shape[0]
    vmem = pl.BlockSpec(memory_space=pltpu.VMEM)
    sem = pltpu.SemaphoreType.DMA
    block = (CELL, lanes)
    fields = jnp.transpose(seam_table, (2, 0, 1))
    out = pl.pallas_call(
        functools.partial(kernel, panels, tiles, sub_rows),
        out_shape=jax.ShapeDtypeStruct((height, width, lanes), F32),
        in_specs=[
            pl.BlockSpec(memory_space=pl.ANY), vmem, pl.BlockSpec(memory_space=pl.ANY), vmem,
        ],
        out_specs=vmem,
        scratch_shapes=[
            pltpu.VMEM((min(sub_rows, SLOTS), cells, cells), BF),
            pltpu.VMEM(((tiles + 1) * sub_rows,) + block, BF),
            pltpu.VMEM((panels - 1, wide) + block, BF),
            pltpu.VMEM((panels, wide) + block, BF),
            pltpu.VMEM((wide,) + block, BF),
            pltpu.VMEM((panels * wide,) + block, BF),
            pltpu.VMEM((tiles - 1, sub_rows) + block, BF),
            pltpu.VMEM((tiles, sub_rows) + block, BF),
            pltpu.VMEM((depth, SUB, 3, SUB, lanes), F32),
            pltpu.VMEM((depth, SUB, 3, SUB, lanes), F32),
            pltpu.VMEM((cells, lanes), F32),
            pltpu.SMEM(fields.shape, jnp.int32),
            sem((min(sub_rows, SLOTS),)), sem((1,)),
            sem((tiles - 1,)), sem((tiles,)),
            sem((panels - 1,)), sem((panels,)),
            sem((panels - 1,)), sem((panels,)),
            sem((tiles - 1,)), sem((tiles,)),
            pltpu.VMEM((6, max(sub_rows - 1, 1)) + block, BF),
            pltpu.VMEM((5, sub_rows) + block, BF),
            pltpu.VMEM((5, sub_rows) + block, BF),
            sem((5,)), sem((5,)), sem((5,)), sem((5,)),
        ],
        compiler_params=pltpu.CompilerParams(
            collective_id=0, has_side_effects=True, vmem_limit_bytes=67043328
        ),
    )(fields, residual[0, 0], inverse[0, 0], blend_weight)
    return out[None, None]


def solution(mesh):
    spec = P("panel", "tile", None, None, None)
    sizes = dict(mesh.shape)
    return jax.shard_map(
        functools.partial(local, sizes["panel"], sizes["tile"]),
        mesh=mesh,
        in_specs=(spec, spec, P(), P()),
        out_specs=spec,
        check_vma=False,
    )
```

```python
import functools

import jax
import jax.numpy as jnp
from jax import lax
from jax.experimental import pallas as pl
from jax.experimental.pallas import tpu as pltpu
from jax.sharding import PartitionSpec as P

TILE_ROWS = 2
SUB = 8
CELL = SUB * SUB
MESH = pl.DeviceIdType.MESH
SLOTS = 4
UNROLLED = 8
BF = jnp.bfloat16
F32 = jnp.float32


def repeat(count, body):
    if count <= UNROLLED:
        for step in range(count):
            body(step)
    else:
        pl.loop(0, count)(body)


def wrapped(index, size):
    return lax.rem(index + size, size)


def pick(options, index):
    out = options[-1]
    for place in range(len(options) - 2, -1, -1):
        out = jnp.where(index == place, options[place], out)
    return out


def kernel(
    panels, tiles, sub_rows,
    seam_in, residual, inverse, blend, out,
    held, shared, window_out, window_in, ghost_out, ghost_in, part_out, part_in,
    ext, spread, weight, seam, inv_sem, seam_sem,
    tile_send, tile_recv, win_send, win_recv, gho_send, gho_recv, par_send, par_recv,
    rest_in, halo_out, halo_in, rest_send, rest_recv, halo_send, halo_recv,
):
    cols = tiles // TILE_ROWS
    side = cols
    depth = sub_rows + 2
    panel, tile = lax.axis_index("panel"), lax.axis_index("tile")
    row, col = lax.div(tile, cols), lax.rem(tile, cols)

    seam_copy = pltpu.make_async_copy(seam_in, seam, seam_sem.at[0])
    seam_copy.start()
    shift = jnp.where(row == 0, 1, 0)
    span = sub_rows + 1
    wide = max(3, span)

    def on_edge(edge, at_row, at_col):
        return pick([at_col == 0, at_row == 0, at_col == cols - 1, at_row == TILE_ROWS - 1], edge)

    def live_edge(of_panel, at_row, at_col):
        across = seam[0, of_panel, 0] >= 0
        edge = jnp.where(across, jnp.where(at_col == 0, 0, 2), jnp.where(at_row == 0, 1, 3))
        return edge, on_edge(edge, at_row, at_col)

    def window_start(edge):
        return jnp.where(lax.rem(edge, 2) == 0, row * sub_rows - 1 + shift, col - 1)

    def window_length(edge):
        return jnp.where(lax.rem(edge, 2) == 0, span, 3)

    def peer(step, way):
        return wrapped(tile + way * (step + 1), tiles)

    near_tiles = ((0, -1), (0, 1), (1, -1), (1, 0), (1, 1))

    def near(slot, action):
        other_row, away = near_tiles[slot]
        at_col = col + away
        target = jnp.where(row == 0, other_row, 1 - other_row) * cols + at_col

        @pl.when((at_col >= 0) & (at_col < cols))
        def _():
            action(target, at_col, near_tiles.index((other_row, -away)))

    def at_side(at_col):
        return (at_col == 0) | (at_col == cols - 1)

    def rim(at_row):
        return jnp.where(at_row == 0, 0, sub_rows - 1)

    def either(test, yes, no):
        pl.when(test)(yes)
        pl.when(jnp.logical_not(test))(no)

    def planned(count, work):
        if count > UNROLLED:
            return work
        ready = [work(k) for k in range(count)]
        return lambda k: ready[k]

    barrier = pltpu.get_barrier_semaphore()

    def greet_tile(step):
        pl.semaphore_signal(
            barrier, inc=1, device_id=(panel, peer(step, 1)), device_id_type=MESH
        )

    repeat(tiles - 1, greet_tile)
    for off in range(1, panels):
        pl.semaphore_signal(
            barrier, inc=1, device_id=(wrapped(panel + off, panels), tile), device_id_type=MESH
        )

    def load_inverse(n):
        slot = lax.rem(n, SLOTS) if not isinstance(n, int) else n % SLOTS
        return pltpu.make_async_copy(inverse.at[n], held.at[slot], inv_sem.at[slot])

    for n in range(min(sub_rows, SLOTS)):
        load_inverse(n).start()

    def own_blocks(j):
        block = residual[pl.ds(j * SUB, SUB)].reshape(CELL, -1)
        shared[tile * sub_rows + j] = block.astype(BF)
        shared[tiles * sub_rows + j] = jnp.zeros(block.shape, BF)

    repeat(sub_rows, own_blocks)
    window_in[panel] = jnp.zeros(window_in.shape[1:], BF)
    ghost_in[pl.ds(panel * wide, wide)] = jnp.zeros((wide,) + ghost_in.shape[1:], BF)
    spread[...] = jnp.zeros_like(spread)
    rest_in[rest_in.shape[0] - 1] = jnp.zeros(rest_in.shape[1:], BF)
    pl.semaphore_wait(barrier, tiles - 1 + panels - 1)

    def tile_copy(step, slot, target, whole):
        at = slot * sub_rows + (0 if whole else rim(lax.div(slot, cols)))
        here = pl.ds(at, sub_rows if whole else 1)
        return pltpu.make_async_remote_copy(
            src_ref=shared.at[here], dst_ref=shared.at[here],
            send_sem=tile_send.at[step], recv_sem=tile_recv.at[slot],
            device_id=(panel, target), device_id_type=MESH,
        )

    def send_tile(step):
        tile_copy(step, tile, peer(step, 1), True).start()

    repeat(tiles - 1, send_tile)

    def rest_copy(slot, target, there):
        here = pl.ds(tile * sub_rows + jnp.where(row == 0, 1, 0), sub_rows - 1)
        return pltpu.make_async_remote_copy(
            src_ref=shared.at[here], dst_ref=rest_in.at[there],
            send_sem=rest_send.at[slot], recv_sem=rest_recv.at[there],
            device_id=(panel, target), device_id_type=MESH,
        )

    def rests(sending, act):
        if sub_rows == 1:
            return
        for slot in range(len(near_tiles)):
            def action(target, at_col, there, slot=slot):
                @pl.when(jnp.logical_not(at_side(col if sending else at_col)))
                def _():
                    act(rest_copy(slot, target, there if sending else slot))

            near(slot, action)


    lanes = residual.shape[-1]
    weight[...] = jnp.transpose(jnp.broadcast_to(blend[...].reshape(1, -1), (lanes, blend.shape[0])))
    seam_copy.wait()
    edge, found = live_edge(panel, row, col)
    neighbour = jnp.maximum(seam[0, panel, edge], 0)
    facing = lax.rem(edge + 2 + seam[1, panel, edge], 4)
    reverse = seam[2, panel, edge]

    def source_cell(ghost):
        i, j = lax.shift_right_logical(ghost, 3), ghost & (SUB - 1)
        d = pick([SUB - 1 - j, SUB - 1 - i, j, i], edge)
        s = jnp.where(lax.rem(edge, 2) == 0, i, j)
        s = jnp.where(reverse > 0, SUB - 1 - s, s)
        across = jnp.where(facing >= 2, SUB - 1 - d, d)
        return jnp.where(lax.rem(facing, 2) == 0, s * SUB + across, across * SUB + s)

    shape = (CELL, CELL)
    first, second = lax.broadcasted_iota(jnp.int32, shape, 0), lax.broadcasted_iota(jnp.int32, shape, 1)
    turn = jnp.where((source_cell(first) == second) & found, 1.0, 0.0).astype(BF)
    turn_back = jnp.where((source_cell(second) == first) & found, 1.0, 0.0).astype(BF)

    def plan_window(off):
        other = wrapped(panel + off, panels)
        its_edge, its_found = live_edge(other, row, col)
        ours = its_found & (seam[0, other, its_edge] == panel)
        my_edge = lax.rem(its_edge + 2 + seam[1, other, its_edge], 4)
        flip = seam[2, other, its_edge]
        start, length = window_start(its_edge), window_length(its_edge)

        def place(k):
            b = start + k
            good = ours & (b >= 0) & (b < side) & (k < length)
            b = jnp.where(flip > 0, side - 1 - b, b)
            at_row = pick([b, 0, b, side - 1], my_edge)
            at_col = pick([0, b, cols - 1, b], my_edge)
            block = (lax.div(at_row, sub_rows) * cols + at_col) * sub_rows + lax.rem(at_row, sub_rows)
            return jnp.where(good, block, tiles * sub_rows)

        return planned(wide, place)

    window_places = [plan_window(off) for off in range(1, panels)]

    def plan_inner(ri):
        places = []
        for ci in range(3):
            at_row, at_col = row * sub_rows + ri - 1, col + ci - 1
            inside = (at_row >= 0) & (at_row < side) & (at_col >= 0) & (at_col < cols)
            at_row = jnp.clip(at_row, 0, side - 1)
            block = (lax.div(at_row, sub_rows) * cols + at_col) * sub_rows + lax.rem(at_row, sub_rows)
            places.append(jnp.where(inside, block, tiles * sub_rows))
        return places

    inner_places = planned(depth, plan_inner)

    low = jnp.where(seam[0, panel, 0] >= 0, 0, 1)
    seams = []
    for own in (low, low + 2):
        far_edge = lax.rem(own + 2 + seam[1, panel, own], 4)
        far_start = window_start(far_edge)
        far_end = jnp.where(on_edge(far_edge, row, col), far_start + window_length(far_edge), -1)
        seams.append((seam[0, panel, own], seam[2, panel, own], far_start, far_end))

    def plan_part(target):
        at_row, at_col = lax.div(target, cols), lax.rem(target, cols)
        its_edge, its_found = live_edge(panel, at_row, at_col)
        other, flip, far_start, far_end = [
            jnp.where(its_edge < 2, lower, upper) for lower, upper in zip(*seams)
        ]

        def place(j):
            b = jnp.where(low == 0, at_row * sub_rows + j, at_col)
            good = its_found & ((low == 0) | (j == rim(at_row)))
            b = jnp.where(flip > 0, side - 1 - b, b)
            good = good & (b >= far_start) & (b < far_end)
            return jnp.where(good, other * wide + b - far_start, panel * wide)

        return planned(sub_rows, place)

    part_places = planned(tiles, lambda step: plan_part(peer(step, 1)))

    def tile_arrival(step):
        source = peer(step, -1)
        tile_copy(step, source, source, True).wait_recv()

    repeat(tiles - 1, tile_arrival)

    def window_copy(off, slot, target):
        return pltpu.make_async_remote_copy(
            src_ref=window_out.at[off - 1], dst_ref=window_in.at[slot],
            send_sem=win_send.at[off - 1], recv_sem=win_recv.at[slot],
            device_id=(target, tile), device_id_type=MESH,
        )

    for off in range(1, panels):
        def fill(k, off=off):
            window_out[off - 1, k] = shared[window_places[off - 1](k)]

        repeat(wide, fill)
        window_copy(off, panel, wrapped(panel + off, panels)).start()


    def inner(ri):
        for ci, place in enumerate(inner_places(ri)):
            ext[ri, :, ci] = shared[place].astype(F32).reshape(SUB, SUB, lanes)

    repeat(depth, inner)

    for off in range(1, panels):
        source = wrapped(panel - off, panels)
        window_copy(off, source, source).wait_recv()

    def outer_side(k):
        block = jnp.dot(turn, window_in[neighbour, k], preferred_element_type=F32)
        block = block.reshape(SUB, SUB, lanes)
        for e, (ri, ci) in enumerate(((k + shift, 0), (0, k), (k + shift, 2), (depth - 1, k))):
            if isinstance(k, int) and k < (3 if e % 2 else span):
                ext[ri, :, ci] += jnp.where(edge == e, block, jnp.zeros_like(block))
            elif not isinstance(k, int) and e % 2 == 0:
                ext[ri, :, ci] += jnp.where(edge == e, block, jnp.zeros_like(block))

    for k in range(3):
        outer_side(k)
    if span > 3:
        repeat(span - 3, lambda k: outer_side(jnp.int32(3) + k))

    def solve(n):
        load_inverse(n).wait()
        slot = n % SLOTS if isinstance(n, int) else lax.rem(n, SLOTS)
        patch = ext[pl.ds(n, 3)].reshape(9 * CELL, lanes).astype(BF)
        solved = jnp.dot(held[slot], patch, preferred_element_type=F32) * weight[...]
        spread[pl.ds(n, 3)] += solved.reshape(3, SUB, 3, SUB, lanes)
        if sub_rows > SLOTS:
            @pl.when(n + SLOTS < sub_rows)
            def _():
                load_inverse(n + SLOTS).start()

    repeat(sub_rows, solve)

    def ghost_copy(off, slot, target):
        return pltpu.make_async_remote_copy(
            src_ref=ghost_out, dst_ref=ghost_in.at[pl.ds(slot * wide, wide)],
            send_sem=gho_send.at[off - 1], recv_sem=gho_recv.at[slot],
            device_id=(target, tile), device_id_type=MESH,
        )

    def ghost(k):
        even = lax.rem(edge, 2) == 0
        ri = jnp.where(even, jnp.minimum(k + shift, depth - 1), jnp.where(edge == 1, 0, depth - 1))
        ci = jnp.where(even, edge, jnp.minimum(k, 2))
        raw = spread[ri, :, ci].reshape(CELL, lanes).astype(BF)
        ghost_out[k] = jnp.dot(turn_back, raw, preferred_element_type=F32).astype(BF)

    repeat(wide, ghost)
    for off in range(1, panels):
        ghost_copy(off, panel, wrapped(panel + off, panels)).start()

    def halo_copy(slot, target, there):
        size = sub_rows if near_tiles[slot][0] == 0 else 1
        return pltpu.make_async_remote_copy(
            src_ref=halo_out.at[slot, pl.ds(0, size)], dst_ref=halo_in.at[there, pl.ds(0, size)],
            send_sem=halo_send.at[slot], recv_sem=halo_recv.at[there],
            device_id=(panel, target), device_id_type=MESH,
        )

    for slot, (other_row, away) in enumerate(near_tiles):
        def send_halo(target, at_col, there, slot=slot, other_row=other_row, away=away):
            def one(j):
                ri = jnp.where(row == 0, depth - 1, 0) if other_row else j + 1
                halo_out[slot, j] = spread[ri, :, away + 1].reshape(CELL, lanes).astype(BF)

            repeat(1 if other_row else sub_rows, one)
            halo_copy(slot, target, there).start()

        near(slot, send_halo)

    def own_part(j):
        out[pl.ds(j * SUB, SUB)] = spread[j + 1, :, 1]

    repeat(sub_rows, own_part)

    for off in range(1, panels):
        source = wrapped(panel - off, panels)
        ghost_copy(off, source, source).wait_recv()

    def part_copy(step, slot, target, whole):
        here = pl.ds(0, sub_rows) if whole else pl.ds(rim(lax.div(target, cols)), 1)
        return pltpu.make_async_remote_copy(
            src_ref=part_out.at[step, here], dst_ref=part_in.at[slot, here],
            send_sem=par_send.at[step], recv_sem=par_recv.at[slot],
            device_id=(panel, target), device_id_type=MESH,
        )

    def send_part(step):
        target = peer(step, 1)

        def one(j):
            part_out[step, j] = ghost_in[part_places(step)(j)]

        repeat(sub_rows, one)
        either(
            at_side(lax.rem(target, cols)),
            lambda: part_copy(step, tile, target, True).start(),
            lambda: part_copy(step, tile, target, False).start(),
        )

    repeat(tiles - 1, send_part)

    def add(j, block):
        out[pl.ds(j * SUB, SUB)] += block.astype(F32).reshape(SUB, SUB, lanes)

    repeat(sub_rows, lambda j: add(j, ghost_in[part_places(tiles - 1)(j)]))

    for slot, (other_row, _) in enumerate(near_tiles):
        def take_halo(target, at_col, there, slot=slot, other_row=other_row):
            halo_copy(slot, target, slot).wait_recv()
            if other_row:
                add(jnp.where(row == 0, sub_rows - 1, 0), halo_in[slot, 0])
            else:
                repeat(sub_rows, lambda j: add(j, halo_in[slot, j]))

        near(slot, take_halo)

    def take_part(step):
        source = peer(step, -1)

        def whole():
            part_copy(step, source, tile, True).wait_recv()
            repeat(sub_rows, lambda j: add(j, part_in[source, j]))

        def outermost():
            part_copy(step, source, tile, False).wait_recv()
            add(rim(row), part_in[source, rim(row)])

        either(at_side(col), whole, outermost)

    repeat(tiles - 1, take_part)

    def sent(step):
        target = peer(step, 1)
        tile_copy(step, tile, target, True).wait_send()
        either(
            at_side(lax.rem(target, cols)),
            lambda: part_copy(step, tile, target, True).wait_send(),
            lambda: part_copy(step, tile, target, False).wait_send(),
        )

    repeat(tiles - 1, sent)
    for slot in range(len(near_tiles)):
        near(slot, lambda target, at_col, there, slot=slot: halo_copy(slot, target, there).wait_send())
    for off in range(1, panels):
        window_copy(off, panel, wrapped(panel + off, panels)).wait_send()
        ghost_copy(off, panel, wrapped(panel + off, panels)).wait_send()


def local(panels, tiles, residual, inverse, blend_weight, seam_table):
    height, width, lanes = residual.shape[2:]
    sub_rows = height // SUB
    depth = sub_rows + 2
    wide = max(3, sub_rows + 1)
    cells = blend_weight.shape[0]
    vmem = pl.BlockSpec(memory_space=pltpu.VMEM)
    sem = pltpu.SemaphoreType.DMA
    block = (CELL, lanes)
    fields = jnp.transpose(seam_table, (2, 0, 1))
    out = pl.pallas_call(
        functools.partial(kernel, panels, tiles, sub_rows),
        out_shape=jax.ShapeDtypeStruct((height, width, lanes), F32),
        in_specs=[
            pl.BlockSpec(memory_space=pl.ANY), vmem, pl.BlockSpec(memory_space=pl.ANY), vmem,
        ],
        out_specs=vmem,
        scratch_shapes=[
            pltpu.VMEM((min(sub_rows, SLOTS), cells, cells), BF),
            pltpu.VMEM(((tiles + 1) * sub_rows,) + block, BF),
            pltpu.VMEM((panels - 1, wide) + block, BF),
            pltpu.VMEM((panels, wide) + block, BF),
            pltpu.VMEM((wide,) + block, BF),
            pltpu.VMEM((panels * wide,) + block, BF),
            pltpu.VMEM((tiles - 1, sub_rows) + block, BF),
            pltpu.VMEM((tiles, sub_rows) + block, BF),
            pltpu.VMEM((depth, SUB, 3, SUB, lanes), F32),
            pltpu.VMEM((depth, SUB, 3, SUB, lanes), F32),
            pltpu.VMEM((cells, lanes), F32),
            pltpu.SMEM(fields.shape, jnp.int32),
            sem((min(sub_rows, SLOTS),)), sem((1,)),
            sem((tiles - 1,)), sem((tiles,)),
            sem((panels - 1,)), sem((panels,)),
            sem((panels - 1,)), sem((panels,)),
            sem((tiles - 1,)), sem((tiles,)),
            pltpu.VMEM((6, max(sub_rows - 1, 1)) + block, BF),
            pltpu.VMEM((5, sub_rows) + block, BF),
            pltpu.VMEM((5, sub_rows) + block, BF),
            sem((5,)), sem((5,)), sem((5,)), sem((5,)),
        ],
        compiler_params=pltpu.CompilerParams(
            collective_id=0, has_side_effects=True, vmem_limit_bytes=67043328
        ),
    )(fields, residual[0, 0], inverse[0, 0], blend_weight)
    return out[None, None]


def solution(mesh):
    spec = P("panel", "tile", None, None, None)
    sizes = dict(mesh.shape)
    return jax.shard_map(
        functools.partial(local, sizes["panel"], sizes["tile"]),
        mesh=mesh,
        in_specs=(spec, spec, P(), P()),
        out_specs=spec,
        check_vma=False,
    )
```
